32 devices in a mesh: grp: 8 (over z, core), blk: 4 (over y, x).
Axes of the slice: x: 2, y: 2, z: 4, core: 2. Of those that a mesh axis runs over, the one named last changes fastest.
Arguments:
- integrals: bfloat16 [8, 128, 128, 128], P(None, 'blk'), may hold values from -0.5 to 0.5
- doubles: bfloat16 [64, 128, 128], P('blk'), may hold values from -0.0059814453 to 0.0059814453
- coulomb: bfloat16 [64, 128, 128], P('blk'), may hold values from -0.1796875 to 0.1796875
- singles: float32 [8, 128], P(None, 'blk'), may hold values from -0.18 to 0.18
- occ_energy: float32 [8], replicated, may hold values from -2 to -0.5
- vir_energy: float32 [128], replicated, may hold values from 0.3 to 3
- triplets: int32 [8, 16, 3], P('grp'), may hold values from 0 to 7
- tile_count: int32 [8], P('grp'), may hold values from 1 to 16, as said below
Outputs:
- triplet_energy: float32 [8, 16], P('grp')
- mean_energy: float32 [], replicated
The draws below stay inside these ranges and needn't reach their ends.
Inputs may be any that keep to these rules, and one draw needn't show every extreme that they name: `tile_count`: slots with an index below a group's count are live; some group has all 16 slots live.
All inputs are finite; a program needn't handle non-finite values.
Results may differ from the reference program's by a relative error of at most 0.0003.
Values may be sent and summed in bfloat16 or wider, within the bound.
A program may use at most 64 MiB of HBM per device.

```python
import jax
import jax.numpy as jnp
from jax import lax

NO = 8
NV = 128
TRIP = 16
GROUPS = 8


def draw_tile_count(key, part):
    key_counts = jax.random.fold_in(key, 11)
    key_full = jax.random.fold_in(key, 12)
    counts = jax.random.randint(key_counts, (GROUPS,), max(1, TRIP // 4), TRIP + 1)
    fullest = jax.random.randint(key_full, (), 0, GROUPS)
    return jnp.where(jnp.arange(GROUPS) == fullest, TRIP, counts).astype(jnp.int32)


def with_ends(drawn, rng, least, top_value):
    place = [jax.random.randint(jax.random.fold_in(rng, axis), (), 0, length) for axis, length in enumerate(drawn.shape)]
    main_axis = drawn.shape.index(max(drawn.shape))
    beside = place[:main_axis] + [(place[main_axis] + 1) % drawn.shape[main_axis]] + place[main_axis + 1:]
    return drawn.at[tuple(place)].set(least).at[tuple(beside)].set(top_value)


def level_of(stream_key, extent, split, smallest, high):
    factor_of = 1.0
    for dim, shards_of in split:
        draws = jax.random.uniform(jax.random.fold_in(jax.random.fold_in(stream_key, 6), dim), (shards_of,), jnp.float32, smallest / len(split), high / len(split))
        factor_of = factor_of * jnp.repeat(jnp.exp(draws), extent[dim] // shards_of).reshape((-1,) + (1,) * (len(extent) - 1 - dim))
    return factor_of


def gaussian(own_key, shape, deviation, bound, split=(), kind=jnp.bfloat16):
    entries = jax.random.normal(own_key, shape, jnp.float32) * deviation
    if len(split) > 0:
        entries = level_of(own_key, shape, split, -0.22, 0.18) * entries
    return jnp.clip(entries, min=-bound, max=bound).astype(kind)


def setup_inputs(seed: int = 0) -> dict:
    streams_of = jax.random.split(jax.random.key(seed), 9)
    integrals = gaussian(streams_of[0], (NO, NV, NV, NV), NV ** -0.5, 0.5, ((1, 4),))
    doubles = gaussian(streams_of[1], (NO * NO, NV, NV), 0.001, 0.0059814453, ((0, 4),))
    coulomb = gaussian(streams_of[2], (NO * NO, NV, NV), 0.03, 0.1796875, ((0, 4),))
    singles = gaussian(streams_of[3], (NO, NV), 0.03, 0.18, ((1, 4),), jnp.float32)
    occ_energy = jnp.clip(jax.random.uniform(streams_of[4], (NO,), jnp.float32, -2.0, -0.5), -2.0, -0.5)
    vir_energy = jnp.clip(jax.random.uniform(streams_of[5], (NV,), jnp.float32, 0.3, 3.0), 0.3, 3.0)
    triplets = with_ends(jax.random.randint(streams_of[6], (GROUPS, TRIP, 3), 0, NO), jax.random.fold_in(streams_of[6], 1), 0, NO - 1).astype(jnp.int32)
    tile_count = draw_tile_count(jax.random.fold_in(streams_of[8], 71), 0)
    return dict(integrals=integrals, doubles=doubles, coulomb=coulomb, singles=singles, occ_energy=occ_energy, vir_energy=vir_energy, triplets=triplets, tile_count=tile_count)


def slot_energy(integrals, doubles, coulomb, singles, occ_energy, vir_energy, triplet):
    first_occ = triplet[0]
    second_occ = triplet[1]
    third_occ = triplet[2]
    slab_rows = integrals[first_occ].reshape(NV * NV, NV)
    doubles_kj = doubles[third_occ * NO + second_occ]
    doubles_jk = doubles[second_occ * NO + third_occ]
    first = jnp.dot(slab_rows, doubles_kj.T, preferred_element_type=jnp.float32).reshape(NV, NV, NV)
    second = jnp.dot(slab_rows, doubles_jk.T, preferred_element_type=jnp.float32).reshape(NV, NV, NV)
    connected = first + jnp.transpose(second, (0, 2, 1))
    coupling = coulomb[second_occ * NO + third_occ].astype(jnp.float32)
    full = connected + singles[first_occ][:, None, None] * coupling[None, :, :]
    occ_sum = occ_energy[first_occ] + occ_energy[second_occ] + occ_energy[third_occ]
    denominator = occ_sum - vir_energy[:, None, None] - vir_energy[None, :, None] - vir_energy[None, None, :]
    return jnp.sum(full * full / denominator)


def reference(integrals, doubles, coulomb, singles, occ_energy, vir_energy, triplets, tile_count):
    flat_triplets = triplets.reshape(GROUPS * TRIP, 3)

    def one_slot(triplet):
        return slot_energy(integrals, doubles, coulomb, singles, occ_energy, vir_energy, triplet)

    energies = lax.map(one_slot, flat_triplets).reshape(GROUPS, TRIP)
    slot_ids = jnp.arange(TRIP, dtype=jnp.int32)
    live = slot_ids[None, :] < tile_count[:, None]
    triplet_energy = jnp.where(live, energies, jnp.zeros_like(energies))
    mean_energy = jnp.sum(triplet_energy) / (GROUPS * TRIP)
    return triplet_energy, mean_energy
```

```python
import functools

import jax
import jax.numpy as jnp
from jax import lax
from jax.experimental import pallas as pl
from jax.experimental.pallas import tpu as pltpu
from jax.sharding import PartitionSpec as P

MESH = pl.DeviceIdType.MESH


def team_count(occupied, rows, groups):
    teams = occupied
    while teams > 1 and (occupied % teams or rows % teams or groups % (2 * teams)):
        teams -= 1
    return teams


def gather_kernel(n, groups, teams, occupied, doubles_ref, coulomb_ref, codes_ref, dp_ref, cp_ref, all_ref,
                  local_sem, send_sem, recv_sem, fsend_sem, frecv_sem, csend_sem, crecv_sem):
    g = lax.axis_index("grp")
    q = lax.axis_index("blk")
    rows, width = doubles_ref.shape[0], doubles_ref.shape[1]
    runs = rows // teams
    half = width // 2
    team = g // (groups // teams)
    core = g % 2
    partner = g + 1 - 2 * core
    mine = pl.ds(pl.multiple_of(core * half, half), half)
    arrays = ((doubles_ref, dp_ref), (coulomb_ref, cp_ref))

    barrier = pltpu.get_barrier_semaphore()
    for dg in range(1, groups):
        pl.semaphore_signal(barrier, inc=1, device_id={"grp": (g + dg) % groups}, device_id_type=MESH)
    for dq in range(1, n):
        pl.semaphore_signal(barrier, inc=1, device_id={"blk": (q + dq) % n}, device_id_type=MESH)

    def own_row(m):
        j = (q * rows + teams * m) // occupied
        return teams * m + (team + occupied * teams - j) % teams

    locals_ = []
    for m in range(runs):
        for x, (src, dst) in enumerate(arrays):
            copy = pltpu.make_async_copy(src.at[own_row(m)], dst.at[q * runs + m], local_sem.at[m, x])
            copy.start()
            locals_.append(copy)
    all_ref[pl.ds(g, 1)] = codes_ref[...]
    pl.semaphore_wait(barrier, groups - 1 + n - 1)

    code_copies = []
    for dg in range(1, groups):
        copy = pltpu.make_async_remote_copy(
            src_ref=codes_ref.at[0], dst_ref=all_ref.at[g], send_sem=csend_sem.at[dg - 1], recv_sem=crecv_sem.at[dg - 1],
            device_id={"grp": (g + dg) % groups}, device_id_type=MESH)
        copy.start()
        code_copies.append(copy)
    sends = []
    for m in range(runs):
        for x, (src, dst) in enumerate(arrays):
            for dq in range(1, n):
                copy = pltpu.make_async_remote_copy(
                    src_ref=src.at[own_row(m), mine], dst_ref=dst.at[q * runs + m, mine],
                    send_sem=send_sem.at[m, x, dq - 1], recv_sem=recv_sem.at[m, x, dq - 1],
                    device_id={"blk": (q + dq) % n}, device_id_type=MESH)
                copy.start()
                sends.append(copy)
    forwards = []
    at = 0
    for m in range(runs):
        for x, (src, dst) in enumerate(arrays):
            for dq in range(1, n):
                sends[at].wait_recv()
                at += 1
                piece = dst.at[((q + n - dq) % n) * runs + m, mine]
                copy = pltpu.make_async_remote_copy(
                    src_ref=piece, dst_ref=piece,
                    send_sem=fsend_sem.at[m, x, dq - 1], recv_sem=frecv_sem.at[m, x, dq - 1],
                    device_id={"grp": partner}, device_id_type=MESH)
                copy.start()
                forwards.append(copy)
    for copy in locals_:
        copy.wait()
    for copy in sends:
        copy.wait_send()
    for copy in forwards:
        copy.wait()
    for copy in code_copies:
        copy.wait()


def compute_kernel(groups, slots, teams, occupied, unroll, codes, singles, occ, vir, integrals_ref, dp_ref, cp_ref,
                   row_ref, out_ref, vbc_ref, slab_ref, list_g, list_s, sems):
    g = lax.axis_index("grp")
    q = lax.axis_index("blk")
    size = groups // teams
    team, member = g // size, g % size
    blocks, width = integrals_ref.shape[1], integrals_ref.shape[2]

    def scan(index, carry):
        count, turn = carry
        other = index // slots
        slot = index % slots
        ours = codes[other, 0, 3 * slots + slot] == team
        list_g[count] = other
        list_s[count] = slot
        take = jnp.logical_and(ours, turn == member)
        after = jnp.where(turn + 1 == size, 0, turn + 1)
        return count + take.astype(jnp.int32), jnp.where(ours, after, turn)

    count, _ = lax.fori_loop(0, groups * slots, scan, (jnp.int32(0), jnp.int32(0)), unroll=4)

    def fetch(at, buf):
        i = codes[list_g[at], 0, list_s[at]]
        return pltpu.make_async_copy(integrals_ref.at[i], slab_ref.at[buf], sems.at[buf])

    @pl.when(count > 0)
    def _():
        fetch(0, 0).start()

    across = jnp.broadcast_to(row_ref[...], (width, width))
    vbc_ref[...] = across + across.T
    out_ref[...] = jnp.zeros_like(out_ref)
    rows = lax.broadcasted_iota(jnp.int32, out_ref.shape, 0)
    lanes = lax.broadcasted_iota(jnp.int32, out_ref.shape, 1)
    contract = (((1,), (1,)), ((), ()))

    def step(at, carry):
        buf = at % 2
        other, slot = list_g[at], list_s[at]
        i = codes[other, 0, slot]
        j = codes[other, 0, slots + slot]
        k = codes[other, 0, 2 * slots + slot]
        jk = (j * occupied + k) // teams
        kj = (k * occupied + j) // teams
        occ_sum = occ[i] + occ[j] + occ[k]

        @pl.when(at + 1 < count)
        def _():
            fetch(at + 1, 1 - buf).start()

        fetch(at, buf).wait()
        d_jk = dp_ref[jk]
        d_kj = dp_ref[kj]

        def one(a, total):
            block = slab_ref[buf, a]
            left = jnp.concatenate([block, d_jk], axis=1)
            right = jnp.concatenate([d_kj, block], axis=1)
            connected = lax.dot_general(left, right, contract, preferred_element_type=jnp.float32)
            full = connected + singles[i, a] * cp_ref[jk].astype(jnp.float32)
            denominator = (occ_sum - vir[q * blocks + a]) - vbc_ref[...]
            value = full * full / denominator
            return total + jnp.sum(value.reshape(width // 8, 8, width), axis=0)

        total = lax.fori_loop(0, blocks, one, jnp.zeros((8, width), jnp.float32), unroll=unroll)
        here = jnp.logical_and(rows == other, lanes == slot)
        out_ref[...] += jnp.where(here, jnp.sum(total), 0.0)
        return carry

    lax.fori_loop(0, count, step, 0)


def reduce_kernel(n, groups, slots, part_ref, trip_ref, mean_ref, blk_buf, grp_buf, send_sem, recv_sem, gsend_sem, grecv_sem,
                  stage_ref):
    g = lax.axis_index("grp")
    q = lax.axis_index("blk")
    barrier = pltpu.get_barrier_semaphore()
    for dg in range(1, groups):
        pl.semaphore_signal(barrier, inc=1, device_id={"grp": (g + dg) % groups}, device_id_type=MESH)
    for dq in range(1, n):
        pl.semaphore_signal(barrier, inc=1, device_id={"blk": (q + dq) % n}, device_id_type=MESH)
    pl.semaphore_wait(barrier, groups - 1 + n - 1)
    copies = []
    for dq in range(1, n):
        copy = pltpu.make_async_remote_copy(
            src_ref=part_ref, dst_ref=blk_buf.at[q], send_sem=send_sem.at[dq - 1], recv_sem=recv_sem.at[dq - 1],
            device_id={"blk": (q + dq) % n}, device_id_type=MESH)
        copy.start()
        copies.append(copy)
    blk_buf[q] = part_ref[...]
    for copy in copies:
        copy.wait()
    stage = jnp.sum(blk_buf[...], axis=0)
    stage_ref[...] = stage
    grp_buf[g] = stage
    copies = []
    for dg in range(1, groups):
        copy = pltpu.make_async_remote_copy(
            src_ref=stage_ref, dst_ref=grp_buf.at[g], send_sem=gsend_sem.at[dg - 1], recv_sem=grecv_sem.at[dg - 1],
            device_id={"grp": (g + dg) % groups}, device_id_type=MESH)
        copy.start()
        copies.append(copy)
    for copy in copies:
        copy.wait()
    table = jnp.sum(grp_buf[...], axis=0)
    rows = lax.broadcasted_iota(jnp.int32, table.shape, 0)
    trip_ref[...] = jnp.sum(jnp.where(rows == g, table, 0.0), axis=0, keepdims=True)
    mean_ref[...] = jnp.sum(table, keepdims=True) / (groups * slots)


def body(n, groups, integrals, doubles, coulomb, singles, occ_energy, vir_energy, triplets, tile_count):
    occupied, _, width, _ = integrals.shape
    rows = doubles.shape[0]
    slots = triplets.shape[1]
    teams = team_count(occupied, rows, groups)
    runs = rows // teams
    pairs = n * runs
    f32, i32 = jnp.float32, jnp.int32
    vmem = pl.BlockSpec(memory_space=pltpu.VMEM)
    smem = pl.BlockSpec(memory_space=pltpu.SMEM)
    hbm = pl.BlockSpec(memory_space=pl.ANY)
    dma = pltpu.SemaphoreType.DMA

    indices = triplets[0].T
    live = jnp.arange(slots, dtype=i32) < tile_count[0]
    team = jnp.where(live, (indices[1] + indices[2]) % teams, -1)
    codes = jnp.concatenate([indices, team[None]], axis=0).reshape(1, 1, 4 * slots)
    lanes = -(-4 * slots // 128) * 128
    codes = jnp.pad(codes, ((0, 0), (0, 0), (0, lanes - 4 * slots)))

    packed = jax.ShapeDtypeStruct((pairs, width, width), doubles.dtype)
    dp, cp, codes_all = pl.pallas_call(
        functools.partial(gather_kernel, n, groups, teams, occupied),
        out_shape=(packed, packed, jax.ShapeDtypeStruct((groups, 1, lanes), i32)),
        in_specs=[hbm, hbm, vmem],
        out_specs=(vmem, vmem, vmem),
        scratch_shapes=[
            dma((runs, 2)), dma((runs, 2, n - 1)), dma((runs, 2, n - 1)), dma((runs, 2, n - 1)), dma((runs, 2, n - 1)),
            dma((groups - 1,)), dma((groups - 1,)),
        ],
        compiler_params=pltpu.CompilerParams(collective_id=0, has_side_effects=True),
        name="gather",
    )(doubles, coulomb, codes)

    blocks = integrals.shape[1]
    part = pl.pallas_call(
        functools.partial(compute_kernel, groups, slots, teams, occupied, 4),
        out_shape=jax.ShapeDtypeStruct((groups, slots), f32),
        in_specs=[smem, smem, smem, smem, hbm, vmem, vmem, vmem],
        out_specs=vmem,
        scratch_shapes=[
            pltpu.VMEM((width, width), f32), pltpu.VMEM((2, blocks, width, width), integrals.dtype),
            pltpu.SMEM((groups * slots + 1,), i32), pltpu.SMEM((groups * slots + 1,), i32), dma((2,)),
        ],
        name="energy",
    )(codes_all, singles, occ_energy, vir_energy, integrals, dp, cp, vir_energy.reshape(1, width))

    trip, mean = pl.pallas_call(
        functools.partial(reduce_kernel, n, groups, slots),
        out_shape=(jax.ShapeDtypeStruct((1, slots), f32), jax.ShapeDtypeStruct((1, 1), f32)),
        in_specs=[vmem],
        out_specs=(vmem, vmem),
        scratch_shapes=[
            pltpu.VMEM((n, groups, slots), f32), pltpu.VMEM((groups, groups, slots), f32),
            dma((n - 1,)), dma((n - 1,)), dma((groups - 1,)), dma((groups - 1,)), pltpu.VMEM((groups, slots), f32),
        ],
        compiler_params=pltpu.CompilerParams(collective_id=1, has_side_effects=True),
        name="join",
    )(part)
    return trip, mean.reshape(())


def solution(mesh):
    in_specs = (
        P(None, "blk", None, None),
        P("blk", None, None),
        P("blk", None, None),
        P(None, "blk"),
        P(),
        P(),
        P("grp", None, None),
        P("grp"),
    )
    out_specs = (P("grp", None), P())
    step = functools.partial(body, mesh.shape["blk"], mesh.shape["grp"])
    return jax.shard_map(step, mesh=mesh, in_specs=in_specs, out_specs=out_specs, check_vma=False)
```

```python
import functools

import jax
import jax.numpy as jnp
from jax import lax
from jax.experimental import pallas as pl
from jax.experimental.pallas import tpu as pltpu
from jax.sharding import PartitionSpec as P

MESH = pl.DeviceIdType.MESH


def team_count(occupied, rows, groups):
    teams = occupied
    while teams > 1 and (occupied % teams or rows % teams or groups % (2 * teams)):
        teams -= 1
    return teams


def gather_kernel(n, groups, teams, occupied, doubles_ref, coulomb_ref, codes_ref, dp_ref, cp_ref, all_ref,
                  local_sem, send_sem, recv_sem, fsend_sem, frecv_sem, csend_sem, crecv_sem):
    g = lax.axis_index("grp")
    q = lax.axis_index("blk")
    rows, width = doubles_ref.shape[0], doubles_ref.shape[1]
    runs = rows // teams
    half = width // 2
    team = g // (groups // teams)
    core = g % 2
    partner = g + 1 - 2 * core
    mine = pl.ds(pl.multiple_of(core * half, half), half)
    arrays = ((doubles_ref, dp_ref), (coulomb_ref, cp_ref))

    barrier = pltpu.get_barrier_semaphore()
    for dg in range(1, groups):
        pl.semaphore_signal(barrier, inc=1, device_id={"grp": (g + dg) % groups}, device_id_type=MESH)
    for dq in range(1, n):
        pl.semaphore_signal(barrier, inc=1, device_id={"blk": (q + dq) % n}, device_id_type=MESH)

    def own_row(m):
        j = (q * rows + teams * m) // occupied
        return teams * m + (team + occupied * teams - j) % teams

    locals_ = []
    for m in range(runs):
        for x, (src, dst) in enumerate(arrays):
            copy = pltpu.make_async_copy(src.at[own_row(m)], dst.at[q * runs + m], local_sem.at[m, x])
            copy.start()
            locals_.append(copy)
    all_ref[pl.ds(g, 1)] = codes_ref[...]
    pl.semaphore_wait(barrier, groups - 1 + n - 1)

    code_copies = []
    for dg in range(1, groups):
        copy = pltpu.make_async_remote_copy(
            src_ref=codes_ref.at[0], dst_ref=all_ref.at[g], send_sem=csend_sem.at[dg - 1], recv_sem=crecv_sem.at[dg - 1],
            device_id={"grp": (g + dg) % groups}, device_id_type=MESH)
        copy.start()
        code_copies.append(copy)
    sends = []
    for m in range(runs):
        for x, (src, dst) in enumerate(arrays):
            for dq in range(1, n):
                copy = pltpu.make_async_remote_copy(
                    src_ref=src.at[own_row(m), mine], dst_ref=dst.at[q * runs + m, mine],
                    send_sem=send_sem.at[m, x, dq - 1], recv_sem=recv_sem.at[m, x, dq - 1],
                    device_id={"blk": (q + dq) % n}, device_id_type=MESH)
                copy.start()
                sends.append(copy)
    forwards = []
    at = 0
    for m in range(runs):
        for x, (src, dst) in enumerate(arrays):
            for dq in range(1, n):
                sends[at].wait_recv()
                at += 1
                piece = dst.at[((q + n - dq) % n) * runs + m, mine]
                copy = pltpu.make_async_remote_copy(
                    src_ref=piece, dst_ref=piece,
                    send_sem=fsend_sem.at[m, x, dq - 1], recv_sem=frecv_sem.at[m, x, dq - 1],
                    device_id={"grp": partner}, device_id_type=MESH)
                copy.start()
                forwards.append(copy)
    for copy in locals_:
        copy.wait()
    for copy in sends:
        copy.wait_send()
    for copy in forwards:
        copy.wait()
    for copy in code_copies:
        copy.wait()


def compute_kernel(groups, slots, teams, occupied, unroll, codes, singles, occ, vir, integrals_ref, dp_ref, cp_ref,
                   row_ref, out_ref, vbc_ref, slab_ref, list_g, list_s, sems):
    g = lax.axis_index("grp")
    q = lax.axis_index("blk")
    size = groups // teams
    team, member = g // size, g % size
    blocks, width = integrals_ref.shape[1], integrals_ref.shape[2]

    def scan(index, carry):
        count, turn = carry
        other = index // slots
        slot = index % slots
        ours = codes[other, 0, 3 * slots + slot] == team
        list_g[count] = other
        list_s[count] = slot
        take = jnp.logical_and(ours, turn == member)
        after = jnp.where(turn + 1 == size, 0, turn + 1)
        return count + take.astype(jnp.int32), jnp.where(ours, after, turn)

    count, _ = lax.fori_loop(0, groups * slots, scan, (jnp.int32(0), jnp.int32(0)), unroll=4)

    def fetch(at, buf):
        i = codes[list_g[at], 0, list_s[at]]
        return pltpu.make_async_copy(integrals_ref.at[i], slab_ref.at[buf], sems.at[buf])

    @pl.when(count > 0)
    def _():
        fetch(0, 0).start()

    across = jnp.broadcast_to(row_ref[...], (width, width))
    vbc_ref[...] = across + across.T
    out_ref[...] = jnp.zeros_like(out_ref)
    rows = lax.broadcasted_iota(jnp.int32, out_ref.shape, 0)
    lanes = lax.broadcasted_iota(jnp.int32, out_ref.shape, 1)
    contract = (((1,), (1,)), ((), ()))

    def step(at, carry):
        buf = at % 2
        other, slot = list_g[at], list_s[at]
        i = codes[other, 0, slot]
        j = codes[other, 0, slots + slot]
        k = codes[other, 0, 2 * slots + slot]
        jk = (j * occupied + k) // teams
        kj = (k * occupied + j) // teams
        occ_sum = occ[i] + occ[j] + occ[k]

        @pl.when(at + 1 < count)
        def _():
            fetch(at + 1, 1 - buf).start()

        fetch(at, buf).wait()
        d_jk = dp_ref[jk]
        d_kj = dp_ref[kj]

        def one(a, total):
            block = slab_ref[buf, a]
            left = jnp.concatenate([block, d_jk], axis=1)
            right = jnp.concatenate([d_kj, block], axis=1)
            connected = lax.dot_general(left, right, contract, preferred_element_type=jnp.float32)
            full = connected + singles[i, a] * cp_ref[jk].astype(jnp.float32)
            denominator = (occ_sum - vir[q * blocks + a]) - vbc_ref[...]
            value = full * full / denominator
            return total + jnp.sum(value.reshape(width // 8, 8, width), axis=0)

        total = lax.fori_loop(0, blocks, one, jnp.zeros((8, width), jnp.float32), unroll=unroll)
        here = jnp.logical_and(rows == other, lanes == slot)
        out_ref[...] += jnp.where(here, jnp.sum(total), 0.0)
        return carry

    lax.fori_loop(0, count, step, 0)


def reduce_kernel(n, groups, slots, part_ref, trip_ref, mean_ref, blk_buf, grp_buf, send_sem, recv_sem, gsend_sem, grecv_sem,
                  stage_ref):
    g = lax.axis_index("grp")
    q = lax.axis_index("blk")
    barrier = pltpu.get_barrier_semaphore()
    for dg in range(1, groups):
        pl.semaphore_signal(barrier, inc=1, device_id={"grp": (g + dg) % groups}, device_id_type=MESH)
    for dq in range(1, n):
        pl.semaphore_signal(barrier, inc=1, device_id={"blk": (q + dq) % n}, device_id_type=MESH)
    pl.semaphore_wait(barrier, groups - 1 + n - 1)
    copies = []
    for dq in range(1, n):
        copy = pltpu.make_async_remote_copy(
            src_ref=part_ref, dst_ref=blk_buf.at[q], send_sem=send_sem.at[dq - 1], recv_sem=recv_sem.at[dq - 1],
            device_id={"blk": (q + dq) % n}, device_id_type=MESH)
        copy.start()
        copies.append(copy)
    blk_buf[q] = part_ref[...]
    for copy in copies:
        copy.wait()
    stage = jnp.sum(blk_buf[...], axis=0)
    stage_ref[...] = stage
    grp_buf[g] = stage
    copies = []
    for dg in range(1, groups):
        copy = pltpu.make_async_remote_copy(
            src_ref=stage_ref, dst_ref=grp_buf.at[g], send_sem=gsend_sem.at[dg - 1], recv_sem=grecv_sem.at[dg - 1],
            device_id={"grp": (g + dg) % groups}, device_id_type=MESH)
        copy.start()
        copies.append(copy)
    for copy in copies:
        copy.wait()
    table = jnp.sum(grp_buf[...], axis=0)
    rows = lax.broadcasted_iota(jnp.int32, table.shape, 0)
    trip_ref[...] = jnp.sum(jnp.where(rows == g, table, 0.0), axis=0, keepdims=True)
    mean_ref[...] = jnp.sum(table, keepdims=True) / (groups * slots)


def body(n, groups, integrals, doubles, coulomb, singles, occ_energy, vir_energy, triplets, tile_count):
    occupied, _, width, _ = integrals.shape
    rows = doubles.shape[0]
    slots = triplets.shape[1]
    teams = team_count(occupied, rows, groups)
    runs = rows // teams
    pairs = n * runs
    f32, i32 = jnp.float32, jnp.int32
    vmem = pl.BlockSpec(memory_space=pltpu.VMEM)
    smem = pl.BlockSpec(memory_space=pltpu.SMEM)
    hbm = pl.BlockSpec(memory_space=pl.ANY)
    dma = pltpu.SemaphoreType.DMA

    indices = triplets[0].T
    live = jnp.arange(slots, dtype=i32) < tile_count[0]
    team = jnp.where(live, (indices[1] + indices[2]) % teams, -1)
    codes = jnp.concatenate([indices, team[None]], axis=0).reshape(1, 1, 4 * slots)
    lanes = -(-4 * slots // 128) * 128
    codes = jnp.pad(codes, ((0, 0), (0, 0), (0, lanes - 4 * slots)))

    packed = jax.ShapeDtypeStruct((pairs, width, width), doubles.dtype)
    dp, cp, codes_all = pl.pallas_call(
        functools.partial(gather_kernel, n, groups, teams, occupied),
        out_shape=(packed, packed, jax.ShapeDtypeStruct((groups, 1, lanes), i32)),
        in_specs=[hbm, hbm, vmem],
        out_specs=(vmem, vmem, vmem),
        scratch_shapes=[
            dma((runs, 2)), dma((runs, 2, n - 1)), dma((runs, 2, n - 1)), dma((runs, 2, n - 1)), dma((runs, 2, n - 1)),
            dma((groups - 1,)), dma((groups - 1,)),
        ],
        compiler_params=pltpu.CompilerParams(collective_id=0, has_side_effects=True),
        name="gather",
    )(doubles, coulomb, codes)

    blocks = integrals.shape[1]
    part = pl.pallas_call(
        functools.partial(compute_kernel, groups, slots, teams, occupied, blocks),
        out_shape=jax.ShapeDtypeStruct((groups, slots), f32),
        in_specs=[smem, smem, smem, smem, hbm, vmem, vmem, vmem],
        out_specs=vmem,
        scratch_shapes=[
            pltpu.VMEM((width, width), f32), pltpu.VMEM((2, blocks, width, width), integrals.dtype),
            pltpu.SMEM((groups * slots + 1,), i32), pltpu.SMEM((groups * slots + 1,), i32), dma((2,)),
        ],
        name="energy",
    )(codes_all, singles, occ_energy, vir_energy, integrals, dp, cp, vir_energy.reshape(1, width))

    trip, mean = pl.pallas_call(
        functools.partial(reduce_kernel, n, groups, slots),
        out_shape=(jax.ShapeDtypeStruct((1, slots), f32), jax.ShapeDtypeStruct((1, 1), f32)),
        in_specs=[vmem],
        out_specs=(vmem, vmem),
        scratch_shapes=[
            pltpu.VMEM((n, groups, slots), f32), pltpu.VMEM((groups, groups, slots), f32),
            dma((n - 1,)), dma((n - 1,)), dma((groups - 1,)), dma((groups - 1,)), pltpu.VMEM((groups, slots), f32),
        ],
        compiler_params=pltpu.CompilerParams(collective_id=1, has_side_effects=True),
        name="join",
    )(part)
    return trip, mean.reshape(())


def solution(mesh):
    in_specs = (
        P(None, "blk", None, None),
        P("blk", None, None),
        P("blk", None, None),
        P(None, "blk"),
        P(),
        P(),
        P("grp", None, None),
        P("grp"),
    )
    out_specs = (P("grp", None), P())
    step = functools.partial(body, mesh.shape["blk"], mesh.shape["grp"])
    return jax.shard_map(step, mesh=mesh, in_specs=in_specs, out_specs=out_specs, check_vma=False)
```

```python
import functools

import jax
import jax.numpy as jnp
from jax import lax
from jax.experimental import pallas as pl
from jax.experimental.pallas import tpu as pltpu
from jax.sharding import PartitionSpec as P

MESH = pl.DeviceIdType.MESH


def team_count(occupied, rows, groups):
    teams = occupied
    while teams > 1 and (occupied % teams or rows % teams or groups % (2 * teams)):
        teams -= 1
    return teams


def gather_kernel(n, groups, teams, occupied, slots, doubles_ref, coulomb_ref, integrals_ref, trip_ref, live_ref, dp_ref, cp_ref,
                  held_ref, list_ref, count_ref, all_ref, held_sem, local_sem, send_sem, recv_sem, fsend_sem, frecv_sem, csend_sem, crecv_sem):
    g = lax.axis_index("grp")
    q = lax.axis_index("blk")
    rows, width = doubles_ref.shape[0], doubles_ref.shape[1]
    runs = rows // teams
    half = width // 2
    team = g // (groups // teams)
    core = g % 2
    partner = g + 1 - 2 * core
    mine = pl.ds(pl.multiple_of(core * half, half), half)
    arrays = ((doubles_ref, dp_ref), (coulomb_ref, cp_ref))

    barrier = pltpu.get_barrier_semaphore()
    for dg in range(1, groups):
        pl.semaphore_signal(barrier, inc=1, device_id={"grp": (g + dg) % groups}, device_id_type=MESH)
    for dq in range(1, n):
        pl.semaphore_signal(barrier, inc=1, device_id={"blk": (q + dq) % n}, device_id_type=MESH)

    def own_row(m):
        j = (q * rows + teams * m) // occupied
        return teams * m + (team + occupied * teams - j) % teams

    locals_ = []
    for m in range(runs):
        for x, (src, dst) in enumerate(arrays):
            copy = pltpu.make_async_copy(src.at[own_row(m)], dst.at[q * runs + m], local_sem.at[m, x])
            copy.start()
            locals_.append(copy)
    held = pltpu.make_async_copy(integrals_ref, held_ref, held_sem)
    held.start()
    i, j, k = trip_ref[0], trip_ref[1], trip_ref[2]
    cube = occupied * occupied * occupied
    owner = lax.rem(j + k, jnp.full_like(j, teams))
    code = owner * cube + (i * occupied + j) * occupied + k
    live = lax.broadcasted_iota(jnp.int32, code.shape, 1) < live_ref[0]
    all_ref[g] = jnp.full((1, all_ref.shape[2]), -1, jnp.int32)
    all_ref[g, :, :slots] = jnp.where(live, code, -1)
    pl.semaphore_wait(barrier, groups - 1 + n - 1)

    code_copies = []
    for dg in range(1, groups):
        copy = pltpu.make_async_remote_copy(
            src_ref=all_ref.at[g], dst_ref=all_ref.at[g], send_sem=csend_sem.at[dg - 1], recv_sem=crecv_sem.at[dg - 1],
            device_id={"grp": (g + dg) % groups}, device_id_type=MESH)
        copy.start()
        code_copies.append(copy)
    sends = []
    for m in range(runs):
        for x, (src, dst) in enumerate(arrays):
            locals_[m * 2 + x].wait()
            for dq in range(1, n):
                copy = pltpu.make_async_remote_copy(
                    src_ref=dst.at[q * runs + m, mine], dst_ref=dst.at[q * runs + m, mine],
                    send_sem=send_sem.at[m, x, dq - 1], recv_sem=recv_sem.at[m, x, dq - 1],
                    device_id={"blk": (q + dq) % n}, device_id_type=MESH)
                copy.start()
                sends.append(copy)
    for copy in code_copies:
        copy.wait()
    table = all_ref[:, 0, :]
    ours = jnp.logical_and(table >= team * cube, table < (team + 1) * cube).astype(jnp.int32)
    inner = table - team * cube
    group_ids = lax.broadcasted_iota(jnp.int32, (groups, 1), 0)
    totals = jnp.sum(ours, axis=1, keepdims=True)
    before = jnp.zeros((groups, 1), jnp.int32)
    for other in range(groups):
        before += jnp.where(group_ids > other, totals[other:other + 1], 0)
    size = groups // teams
    member = g % size
    places = lax.broadcasted_iota(jnp.int32, (groups, list_ref.shape[1]), 1) * size + member
    listed = jnp.zeros(places.shape, jnp.int32)
    for slot in range(slots):
        column = ours[:, slot:slot + 1]
        value = (group_ids * slots + slot) * cube + inner[:, slot:slot + 1]
        rank = jnp.where(column > 0, before, -1)
        listed += jnp.where(places == rank, value, 0)
        before += column
    list_ref[...] = jnp.sum(listed, axis=0, keepdims=True)
    whole = jnp.sum(totals, axis=0, keepdims=True)
    count_ref[...] = jnp.broadcast_to((whole - member + size - 1) // size, count_ref.shape)

    forwards = []
    at = 0
    for m in range(runs):
        for x, (src, dst) in enumerate(arrays):
            for dq in range(1, n):
                sends[at].wait_recv()
                at += 1
                piece = dst.at[((q + n - dq) % n) * runs + m, mine]
                copy = pltpu.make_async_remote_copy(
                    src_ref=piece, dst_ref=piece,
                    send_sem=fsend_sem.at[m, x, dq - 1], recv_sem=frecv_sem.at[m, x, dq - 1],
                    device_id={"grp": partner}, device_id_type=MESH)
                copy.start()
                forwards.append(copy)
    held.wait()
    for copy in sends:
        copy.wait_send()
    for copy in forwards:
        copy.wait()


def compute_kernel(groups, slots, teams, occupied, unroll, listed, counts, singles, occ, vir, integrals_ref, dp_ref, cp_ref,
                   row_ref, out_ref, vbc_ref):
    q = lax.axis_index("blk")
    blocks, width = integrals_ref.shape[1], integrals_ref.shape[2]
    count = counts[0, 0]

    def decode(at):
        code = listed[0, at]
        k = lax.rem(code, occupied)
        j = lax.rem(lax.div(code, occupied), occupied)
        i = lax.rem(lax.div(code, occupied * occupied), occupied)
        return lax.div(code, occupied * occupied * occupied), i, j, k

    across = jnp.broadcast_to(row_ref[...], (width, width))
    vbc_ref[...] = across + across.T
    out_ref[...] = jnp.zeros_like(out_ref)
    rows = lax.broadcasted_iota(jnp.int32, out_ref.shape, 0)
    lanes = lax.broadcasted_iota(jnp.int32, out_ref.shape, 1)
    contract = (((1,), (1,)), ((), ()))

    def step(at, carry):
        place, i, j, k = decode(at)
        other, slot = lax.div(place, slots), lax.rem(place, slots)
        occ_sum = occ[i] + occ[j] + occ[k]

        jk = lax.div(j * occupied + k, teams)
        kj = lax.div(k * occupied + j, teams)
        d_jk = dp_ref[jk]
        d_kj = dp_ref[kj]

        def one(a, total):
            block = integrals_ref[i, a]
            left = jnp.concatenate([block, d_jk], axis=1)
            right = jnp.concatenate([d_kj, block], axis=1)
            connected = lax.dot_general(left, right, contract, preferred_element_type=jnp.float32)
            full = connected + singles[i, a] * cp_ref[jk].astype(jnp.float32)
            denominator = (occ_sum - vir[q * blocks + a]) - vbc_ref[...]
            value = full * full / denominator
            return total + jnp.sum(value.reshape(width // 8, 8, width), axis=0)

        total = lax.fori_loop(0, blocks, one, jnp.zeros((8, width), jnp.float32), unroll=unroll)
        here = jnp.logical_and(rows == other, lanes == slot)
        out_ref[...] += jnp.where(here, jnp.sum(total), 0.0)
        return carry

    lax.fori_loop(0, count, step, 0)


def reduce_kernel(n, groups, slots, part_ref, trip_ref, mean_ref, blk_buf, grp_buf, send_sem, recv_sem, gsend_sem, grecv_sem,
                  stage_ref):
    g = lax.axis_index("grp")
    q = lax.axis_index("blk")
    barrier = pltpu.get_barrier_semaphore()
    for dg in range(1, groups):
        pl.semaphore_signal(barrier, inc=1, device_id={"grp": (g + dg) % groups}, device_id_type=MESH)
    for dq in range(1, n):
        pl.semaphore_signal(barrier, inc=1, device_id={"blk": (q + dq) % n}, device_id_type=MESH)
    pl.semaphore_wait(barrier, groups - 1 + n - 1)
    copies = []
    for dq in range(1, n):
        copy = pltpu.make_async_remote_copy(
            src_ref=part_ref, dst_ref=blk_buf.at[q], send_sem=send_sem.at[dq - 1], recv_sem=recv_sem.at[dq - 1],
            device_id={"blk": (q + dq) % n}, device_id_type=MESH)
        copy.start()
        copies.append(copy)
    blk_buf[q] = part_ref[...]
    for copy in copies:
        copy.wait()
    stage = jnp.sum(blk_buf[...], axis=0)
    stage_ref[...] = stage
    grp_buf[g] = stage
    copies = []
    for dg in range(1, groups):
        copy = pltpu.make_async_remote_copy(
            src_ref=stage_ref, dst_ref=grp_buf.at[g], send_sem=gsend_sem.at[dg - 1], recv_sem=grecv_sem.at[dg - 1],
            device_id={"grp": (g + dg) % groups}, device_id_type=MESH)
        copy.start()
        copies.append(copy)
    for copy in copies:
        copy.wait()
    table = jnp.sum(grp_buf[...], axis=0)
    rows = lax.broadcasted_iota(jnp.int32, table.shape, 0)
    trip_ref[...] = jnp.sum(jnp.where(rows == g, table, 0.0), axis=0, keepdims=True)
    mean_ref[...] = jnp.sum(table, keepdims=True) / (groups * slots)


def body(n, groups, integrals, doubles, coulomb, singles, occ_energy, vir_energy, triplets, tile_count):
    occupied, _, width, _ = integrals.shape
    rows = doubles.shape[0]
    slots = triplets.shape[1]
    teams = team_count(occupied, rows, groups)
    runs = rows // teams
    pairs = n * runs
    f32, i32 = jnp.float32, jnp.int32
    vmem = pl.BlockSpec(memory_space=pltpu.VMEM)
    smem = pl.BlockSpec(memory_space=pltpu.SMEM)
    hbm = pl.BlockSpec(memory_space=pltpu.HBM)
    dma = pltpu.SemaphoreType.DMA

    row_bytes = pairs * width * width * doubles.dtype.itemsize
    spare = 1 << 20
    keep = integrals.size * integrals.dtype.itemsize + 2 * row_bytes + 2 * spare
    lanes = -(-slots // 128) * 128
    length = -(-groups * slots // 128) * 128

    packed = jax.ShapeDtypeStruct((pairs, width, width), doubles.dtype)
    dp, cp, held, listed, counts = pl.pallas_call(
        functools.partial(gather_kernel, n, groups, teams, occupied, slots),
        out_shape=(packed, packed, jax.ShapeDtypeStruct(integrals.shape, integrals.dtype), jax.ShapeDtypeStruct((1, length), i32), jax.ShapeDtypeStruct((1, 128), i32)),
        in_specs=[hbm, hbm, hbm, vmem, smem],
        out_specs=(vmem, vmem, vmem, vmem, vmem),
        scratch_shapes=[
            pltpu.VMEM((groups, 1, lanes), i32), dma, dma((runs, 2)), dma((runs, 2, n - 1)), dma((runs, 2, n - 1)), dma((runs, 2, n - 1)), dma((runs, 2, n - 1)),
            dma((groups - 1,)), dma((groups - 1,)),
        ],
        compiler_params=pltpu.CompilerParams(collective_id=0, has_side_effects=True, vmem_limit_bytes=keep),
        name="gather",
    )(*(pltpu.with_memory_space_constraint(x, pltpu.HBM) for x in (doubles, coulomb, integrals)), jnp.transpose(triplets, (2, 0, 1)), tile_count)

    blocks = integrals.shape[1]
    part = pl.pallas_call(
        functools.partial(compute_kernel, groups, slots, teams, occupied, blocks),
        out_shape=jax.ShapeDtypeStruct((groups, slots), f32),
        in_specs=[smem, smem, smem, smem, smem, vmem, vmem, vmem, vmem],
        out_specs=vmem,
        scratch_shapes=[pltpu.VMEM((width, width), f32)],
        compiler_params=pltpu.CompilerParams(vmem_limit_bytes=keep),
        name="energy",
    )(listed, counts, singles, occ_energy, vir_energy, held, dp, cp, vir_energy.reshape(1, width))

    trip, mean = pl.pallas_call(
        functools.partial(reduce_kernel, n, groups, slots),
        out_shape=(jax.ShapeDtypeStruct((1, slots), f32), jax.ShapeDtypeStruct((1, 1), f32)),
        in_specs=[vmem],
        out_specs=(vmem, vmem),
        scratch_shapes=[
            pltpu.VMEM((n, groups, slots), f32), pltpu.VMEM((groups, groups, slots), f32),
            dma((n - 1,)), dma((n - 1,)), dma((groups - 1,)), dma((groups - 1,)), pltpu.VMEM((groups, slots), f32),
        ],
        compiler_params=pltpu.CompilerParams(collective_id=1, has_side_effects=True, vmem_limit_bytes=4 * spare),
        name="join",
    )(part)
    return trip, mean.reshape(())


def solution(mesh):
    in_specs = (
        P(None, "blk", None, None),
        P("blk", None, None),
        P("blk", None, None),
        P(None, "blk"),
        P(),
        P(),
        P("grp", None, None),
        P("grp"),
    )
    out_specs = (P("grp", None), P())
    step = functools.partial(body, mesh.shape["blk"], mesh.shape["grp"])
    return jax.shard_map(step, mesh=mesh, in_specs=in_specs, out_specs=out_specs, check_vma=False)
```

```python
import functools

import jax
import jax.numpy as jnp
from jax import lax
from jax.experimental import pallas as pl
from jax.experimental.pallas import tpu as pltpu
from jax.sharding import PartitionSpec as P

MESH = pl.DeviceIdType.MESH


def team_count(occupied, rows, groups):
    teams = occupied
    while teams > 1 and (occupied % teams or rows % teams or groups % (2 * teams)):
        teams -= 1
    return teams


def gather_kernel(n, groups, teams, occupied, slots, doubles_ref, coulomb_ref, integrals_ref, trip_hbm, live_ref, dp_ref, cp_ref,
                  held_ref, list_ref, count_ref, all_ref, trip_ref, small_sem, held_sem, local_sem, send_sem, recv_sem, fsend_sem, frecv_sem, csend_sem, crecv_sem):
    g = lax.axis_index("grp")
    q = lax.axis_index("blk")
    rows, width = doubles_ref.shape[0], doubles_ref.shape[1]
    runs = rows // teams
    half = width // 2
    team = g // (groups // teams)
    core = g % 2
    partner = g + 1 - 2 * core
    mine = pl.ds(pl.multiple_of(core * half, half), half)
    arrays = ((doubles_ref, dp_ref), (coulomb_ref, cp_ref))

    barrier = pltpu.get_barrier_semaphore()
    for dg in range(1, groups):
        pl.semaphore_signal(barrier, inc=1, device_id={"grp": (g + dg) % groups}, device_id_type=MESH)
    for dq in range(1, n):
        pl.semaphore_signal(barrier, inc=1, device_id={"blk": (q + dq) % n}, device_id_type=MESH)

    def own_row(m):
        j = (q * rows + teams * m) // occupied
        return teams * m + (team + occupied * teams - j) % teams

    small = pltpu.make_async_copy(trip_hbm, trip_ref, small_sem)
    small.start()
    locals_ = []
    for m in range(runs):
        for x, (src, dst) in enumerate(arrays):
            copy = pltpu.make_async_copy(src.at[own_row(m)], dst.at[q * runs + m], local_sem.at[m, x])
            copy.start()
            locals_.append(copy)
    held = pltpu.make_async_copy(integrals_ref, held_ref, held_sem)
    held.start()
    small.wait()
    i, j, k = trip_ref[0], trip_ref[1], trip_ref[2]
    cube = occupied * occupied * occupied
    owner = lax.rem(j + k, jnp.full_like(j, teams))
    code = owner * cube + (i * occupied + j) * occupied + k
    live = lax.broadcasted_iota(jnp.int32, code.shape, 1) < live_ref[0]
    all_ref[g] = jnp.full((1, all_ref.shape[2]), -1, jnp.int32)
    all_ref[g, :, :slots] = jnp.where(live, code, -1)
    pl.semaphore_wait(barrier, groups - 1 + n - 1)

    code_copies = []
    for dg in range(1, groups):
        copy = pltpu.make_async_remote_copy(
            src_ref=all_ref.at[g], dst_ref=all_ref.at[g], send_sem=csend_sem.at[dg - 1], recv_sem=crecv_sem.at[dg - 1],
            device_id={"grp": (g + dg) % groups}, device_id_type=MESH)
        copy.start()
        code_copies.append(copy)
    sends = []
    for m in range(runs):
        for x, (src, dst) in enumerate(arrays):
            locals_[m * 2 + x].wait()
            for dq in range(1, n):
                copy = pltpu.make_async_remote_copy(
                    src_ref=dst.at[q * runs + m, mine], dst_ref=dst.at[q * runs + m, mine],
                    send_sem=send_sem.at[m, x, dq - 1], recv_sem=recv_sem.at[m, x, dq - 1],
                    device_id={"blk": (q + dq) % n}, device_id_type=MESH)
                copy.start()
                sends.append(copy)
    for copy in code_copies:
        copy.wait()
    table = all_ref[:, 0, :]
    ours = jnp.logical_and(table >= team * cube, table < (team + 1) * cube).astype(jnp.int32)
    inner = table - team * cube
    group_ids = lax.broadcasted_iota(jnp.int32, (groups, 1), 0)
    totals = jnp.sum(ours, axis=1, keepdims=True)
    before = jnp.zeros((groups, 1), jnp.int32)
    for other in range(groups):
        before += jnp.where(group_ids > other, totals[other:other + 1], 0)
    size = groups // teams
    member = g % size
    places = lax.broadcasted_iota(jnp.int32, (groups, list_ref.shape[1]), 1) * size + member
    listed = jnp.zeros(places.shape, jnp.int32)
    for slot in range(slots):
        column = ours[:, slot:slot + 1]
        value = (group_ids * slots + slot) * cube + inner[:, slot:slot + 1]
        rank = jnp.where(column > 0, before, -1)
        listed += jnp.where(places == rank, value, 0)
        before += column
    list_ref[...] = jnp.sum(listed, axis=0, keepdims=True)
    whole = jnp.sum(totals, axis=0, keepdims=True)
    count_ref[...] = jnp.broadcast_to((whole - member + size - 1) // size, count_ref.shape)

    forwards = []
    at = 0
    for m in range(runs):
        for x, (src, dst) in enumerate(arrays):
            for dq in range(1, n):
                sends[at].wait_recv()
                at += 1
                piece = dst.at[((q + n - dq) % n) * runs + m, mine]
                copy = pltpu.make_async_remote_copy(
                    src_ref=piece, dst_ref=piece,
                    send_sem=fsend_sem.at[m, x, dq - 1], recv_sem=frecv_sem.at[m, x, dq - 1],
                    device_id={"grp": partner}, device_id_type=MESH)
                copy.start()
                forwards.append(copy)
    held.wait()
    for copy in sends:
        copy.wait_send()
    for copy in forwards:
        copy.wait()


def compute_kernel(groups, slots, teams, occupied, unroll, listed, counts, singles, occ, vir, integrals_ref, dp_ref, cp_ref,
                   row_ref, out_ref, vbc_ref):
    q = lax.axis_index("blk")
    blocks, width = integrals_ref.shape[1], integrals_ref.shape[2]
    count = counts[0, 0]

    def decode(at):
        code = listed[0, at]
        k = lax.rem(code, occupied)
        j = lax.rem(lax.div(code, occupied), occupied)
        i = lax.rem(lax.div(code, occupied * occupied), occupied)
        return lax.div(code, occupied * occupied * occupied), i, j, k

    across = jnp.broadcast_to(row_ref[...], (width, width))
    vbc_ref[...] = across + across.T
    out_ref[...] = jnp.zeros_like(out_ref)
    rows = lax.broadcasted_iota(jnp.int32, out_ref.shape, 0)
    lanes = lax.broadcasted_iota(jnp.int32, out_ref.shape, 1)
    contract = (((1,), (1,)), ((), ()))

    def step(at, carry):
        place, i, j, k = decode(at)
        other, slot = lax.div(place, slots), lax.rem(place, slots)
        occ_sum = occ[i] + occ[j] + occ[k]

        jk = lax.div(j * occupied + k, teams)
        kj = lax.div(k * occupied + j, teams)
        d_jk = dp_ref[jk]
        d_kj = dp_ref[kj]

        def one(a, total):
            block = integrals_ref[i, a]
            left = jnp.concatenate([block, d_jk], axis=1)
            right = jnp.concatenate([d_kj, block], axis=1)
            connected = lax.dot_general(left, right, contract, preferred_element_type=jnp.float32)
            full = connected + singles[i, a] * cp_ref[jk].astype(jnp.float32)
            denominator = (occ_sum - vir[q * blocks + a]) - vbc_ref[...]
            value = full * full / denominator
            return total + jnp.sum(value.reshape(width // 8, 8, width), axis=0)

        total = lax.fori_loop(0, blocks, one, jnp.zeros((8, width), jnp.float32), unroll=unroll)
        here = jnp.logical_and(rows == other, lanes == slot)
        out_ref[...] += jnp.where(here, jnp.sum(total), 0.0)
        return carry

    lax.fori_loop(0, count, step, 0)


def reduce_kernel(n, groups, slots, part_ref, trip_ref, mean_ref, blk_buf, grp_buf, send_sem, recv_sem, gsend_sem, grecv_sem,
                  stage_ref):
    g = lax.axis_index("grp")
    q = lax.axis_index("blk")
    barrier = pltpu.get_barrier_semaphore()
    for dg in range(1, groups):
        pl.semaphore_signal(barrier, inc=1, device_id={"grp": (g + dg) % groups}, device_id_type=MESH)
    for dq in range(1, n):
        pl.semaphore_signal(barrier, inc=1, device_id={"blk": (q + dq) % n}, device_id_type=MESH)
    pl.semaphore_wait(barrier, groups - 1 + n - 1)
    copies = []
    for dq in range(1, n):
        copy = pltpu.make_async_remote_copy(
            src_ref=part_ref, dst_ref=blk_buf.at[q], send_sem=send_sem.at[dq - 1], recv_sem=recv_sem.at[dq - 1],
            device_id={"blk": (q + dq) % n}, device_id_type=MESH)
        copy.start()
        copies.append(copy)
    blk_buf[q] = part_ref[...]
    for copy in copies:
        copy.wait()
    stage = jnp.sum(blk_buf[...], axis=0)
    stage_ref[...] = stage
    grp_buf[g] = stage
    copies = []
    for dg in range(1, groups):
        copy = pltpu.make_async_remote_copy(
            src_ref=stage_ref, dst_ref=grp_buf.at[g], send_sem=gsend_sem.at[dg - 1], recv_sem=grecv_sem.at[dg - 1],
            device_id={"grp": (g + dg) % groups}, device_id_type=MESH)
        copy.start()
        copies.append(copy)
    for copy in copies:
        copy.wait()
    table = jnp.sum(grp_buf[...], axis=0)
    rows = lax.broadcasted_iota(jnp.int32, table.shape, 0)
    trip_ref[...] = jnp.sum(jnp.where(rows == g, table, 0.0), axis=0, keepdims=True)
    mean_ref[...] = jnp.sum(table, keepdims=True) / (groups * slots)


def body(n, groups, integrals, doubles, coulomb, singles, occ_energy, vir_energy, triplets, tile_count):
    occupied, _, width, _ = integrals.shape
    rows = doubles.shape[0]
    slots = triplets.shape[1]
    teams = team_count(occupied, rows, groups)
    runs = rows // teams
    pairs = n * runs
    f32, i32 = jnp.float32, jnp.int32
    vmem = pl.BlockSpec(memory_space=pltpu.VMEM)
    smem = pl.BlockSpec(memory_space=pltpu.SMEM)
    hbm = pl.BlockSpec(memory_space=pltpu.HBM)
    dma = pltpu.SemaphoreType.DMA

    row_bytes = pairs * width * width * doubles.dtype.itemsize
    spare = 1 << 20
    keep = integrals.size * integrals.dtype.itemsize + 2 * row_bytes + 2 * spare
    lanes = -(-slots // 128) * 128
    length = -(-groups * slots // 128) * 128

    packed = jax.ShapeDtypeStruct((pairs, width, width), doubles.dtype)
    dp, cp, held, listed, counts = pl.pallas_call(
        functools.partial(gather_kernel, n, groups, teams, occupied, slots),
        out_shape=(packed, packed, jax.ShapeDtypeStruct(integrals.shape, integrals.dtype), jax.ShapeDtypeStruct((1, length), i32), jax.ShapeDtypeStruct((1, 128), i32)),
        in_specs=[hbm, hbm, hbm, hbm, smem],
        out_specs=(vmem, vmem, vmem, vmem, vmem),
        scratch_shapes=[
            pltpu.VMEM((groups, 1, lanes), i32), pltpu.VMEM((3, 1, slots), i32), dma, dma, dma((runs, 2)), dma((runs, 2, n - 1)), dma((runs, 2, n - 1)), dma((runs, 2, n - 1)), dma((runs, 2, n - 1)),
            dma((groups - 1,)), dma((groups - 1,)),
        ],
        compiler_params=pltpu.CompilerParams(collective_id=0, has_side_effects=True, vmem_limit_bytes=keep),
        name="gather",
    )(*(pltpu.with_memory_space_constraint(x, pltpu.HBM)
        for x in (doubles, coulomb, integrals, jnp.transpose(triplets, (2, 0, 1)))), tile_count)

    blocks = integrals.shape[1]
    part = pl.pallas_call(
        functools.partial(compute_kernel, groups, slots, teams, occupied, blocks),
        out_shape=jax.ShapeDtypeStruct((groups, slots), f32),
        in_specs=[smem, smem, smem, smem, smem, vmem, vmem, vmem, vmem],
        out_specs=vmem,
        scratch_shapes=[pltpu.VMEM((width, width), f32)],
        compiler_params=pltpu.CompilerParams(vmem_limit_bytes=keep),
        name="energy",
    )(listed, counts, singles, occ_energy, vir_energy, held, dp, cp, vir_energy.reshape(1, width))

    trip, mean = pl.pallas_call(
        functools.partial(reduce_kernel, n, groups, slots),
        out_shape=(jax.ShapeDtypeStruct((1, slots), f32), jax.ShapeDtypeStruct((1, 1), f32)),
        in_specs=[vmem],
        out_specs=(vmem, vmem),
        scratch_shapes=[
            pltpu.VMEM((n, groups, slots), f32), pltpu.VMEM((groups, groups, slots), f32),
            dma((n - 1,)), dma((n - 1,)), dma((groups - 1,)), dma((groups - 1,)), pltpu.VMEM((groups, slots), f32),
        ],
        compiler_params=pltpu.CompilerParams(collective_id=1, has_side_effects=True, vmem_limit_bytes=4 * spare),
        name="join",
    )(part)
    return trip, mean.reshape(())


def solution(mesh):
    in_specs = (
        P(None, "blk", None, None),
        P("blk", None, None),
        P("blk", None, None),
        P(None, "blk"),
        P(),
        P(),
        P("grp", None, None),
        P("grp"),
    )
    out_specs = (P("grp", None), P())
    step = functools.partial(body, mesh.shape["blk"], mesh.shape["grp"])
    return jax.shard_map(step, mesh=mesh, in_specs=in_specs, out_specs=out_specs, check_vma=False)
```

```python
import functools

import jax
import jax.numpy as jnp
from jax import lax
from jax.experimental import pallas as pl
from jax.experimental.pallas import tpu as pltpu
from jax.sharding import PartitionSpec as P

MESH = pl.DeviceIdType.MESH


def team_count(occupied, rows, groups):
    teams = occupied
    while teams > 1 and (occupied % teams or rows % teams or groups % (2 * teams)):
        teams -= 1
    return teams


def gather_kernel(n, groups, teams, occupied, slots, doubles_ref, coulomb_ref, integrals_ref, trip_hbm, live_ref, dp_ref, cp_ref,
                  held_ref, list_ref, count_ref, all_ref, trip_ref, small_sem, held_sem, local_sem, send_sem, recv_sem, fsend_sem, frecv_sem, csend_sem, crecv_sem):
    g = lax.axis_index("grp")
    q = lax.axis_index("blk")
    rows, width = doubles_ref.shape[0], doubles_ref.shape[1]
    runs = rows // teams
    half = width // 2
    team = g // (groups // teams)
    core = g % 2
    partner = g + 1 - 2 * core
    mine = pl.ds(pl.multiple_of(core * half, half), half)
    arrays = ((doubles_ref, dp_ref), (coulomb_ref, cp_ref))

    barrier = pltpu.get_barrier_semaphore()
    for dg in range(1, groups):
        pl.semaphore_signal(barrier, inc=1, device_id={"grp": (g + dg) % groups}, device_id_type=MESH)
    for dq in range(1, n):
        pl.semaphore_signal(barrier, inc=1, device_id={"blk": (q + dq) % n}, device_id_type=MESH)

    def own_row(m):
        j = (q * rows + teams * m) // occupied
        return teams * m + (team + occupied * teams - j) % teams

    small = pltpu.make_async_copy(trip_hbm, trip_ref, small_sem)
    small.start()
    locals_ = []
    for m in range(runs):
        for x, (src, dst) in enumerate(arrays):
            copy = pltpu.make_async_copy(src.at[own_row(m)], dst.at[q * runs + m], local_sem.at[m, x])
            copy.start()
            locals_.append(copy)
    held = pltpu.make_async_copy(integrals_ref, held_ref, held_sem)
    held.start()
    small.wait()
    i, j, k = trip_ref[0], trip_ref[1], trip_ref[2]
    cube = occupied * occupied * occupied
    owner = lax.rem(j + k, jnp.full_like(j, teams))
    code = owner * cube + (i * occupied + j) * occupied + k
    live = lax.broadcasted_iota(jnp.int32, code.shape, 1) < live_ref[0]
    all_ref[g] = jnp.full((1, all_ref.shape[2]), -1, jnp.int32)
    all_ref[g, :, :slots] = jnp.where(live, code, -1)
    pl.semaphore_wait(barrier, groups - 1 + n - 1)

    code_copies = []
    for dg in range(1, groups):
        copy = pltpu.make_async_remote_copy(
            src_ref=all_ref.at[g], dst_ref=all_ref.at[g], send_sem=csend_sem.at[dg - 1], recv_sem=crecv_sem.at[dg - 1],
            device_id={"grp": (g + dg) % groups}, device_id_type=MESH)
        copy.start()
        code_copies.append(copy)
    sends = []
    for m in range(runs):
        for x, (src, dst) in enumerate(arrays):
            locals_[m * 2 + x].wait()
            for dq in range(1, n):
                copy = pltpu.make_async_remote_copy(
                    src_ref=dst.at[q * runs + m, mine], dst_ref=dst.at[q * runs + m, mine],
                    send_sem=send_sem.at[m, x, dq - 1], recv_sem=recv_sem.at[m, x, dq - 1],
                    device_id={"blk": (q + dq) % n}, device_id_type=MESH)
                copy.start()
                sends.append(copy)
    for copy in code_copies:
        copy.wait()
    table = all_ref[:, 0, :]
    ours = jnp.logical_and(table >= team * cube, table < (team + 1) * cube).astype(jnp.int32)
    inner = table - team * cube
    group_ids = lax.broadcasted_iota(jnp.int32, (groups, 1), 0)
    totals = jnp.sum(ours, axis=1, keepdims=True)
    before = jnp.zeros((groups, 1), jnp.int32)
    for other in range(groups):
        before += jnp.where(group_ids > other, totals[other:other + 1], 0)
    size = groups // teams
    member = g % size
    places = lax.broadcasted_iota(jnp.int32, (groups, list_ref.shape[1]), 1) * size + member
    listed = jnp.zeros(places.shape, jnp.int32)
    for slot in range(slots):
        column = ours[:, slot:slot + 1]
        value = (group_ids * slots + slot) * cube + inner[:, slot:slot + 1]
        rank = jnp.where(column > 0, before, -1)
        listed += jnp.where(places == rank, value, 0)
        before += column
    list_ref[...] = jnp.sum(listed, axis=0, keepdims=True)
    whole = jnp.sum(totals, axis=0, keepdims=True)
    count_ref[...] = jnp.broadcast_to((whole - member + size - 1) // size, count_ref.shape)

    forwards = []
    at = 0
    for m in range(runs):
        for x, (src, dst) in enumerate(arrays):
            for dq in range(1, n):
                sends[at].wait_recv()
                at += 1
                piece = dst.at[((q + n - dq) % n) * runs + m, mine]
                copy = pltpu.make_async_remote_copy(
                    src_ref=piece, dst_ref=piece,
                    send_sem=fsend_sem.at[m, x, dq - 1], recv_sem=frecv_sem.at[m, x, dq - 1],
                    device_id={"grp": partner}, device_id_type=MESH)
                copy.start()
                forwards.append(copy)
    held.wait()
    for copy in sends:
        copy.wait_send()
    for copy in forwards:
        copy.wait()


def compute_kernel(groups, slots, teams, occupied, unroll, listed, counts, singles, occ, vir, integrals_ref, dp_ref, cp_ref,
                   row_ref, out_ref, vbc_ref):
    q = lax.axis_index("blk")
    blocks, width = integrals_ref.shape[1], integrals_ref.shape[2]
    count = counts[0, 0]

    def decode(at):
        code = listed[0, at]
        k = lax.rem(code, occupied)
        j = lax.rem(lax.div(code, occupied), occupied)
        i = lax.rem(lax.div(code, occupied * occupied), occupied)
        return lax.div(code, occupied * occupied * occupied), i, j, k

    across = jnp.broadcast_to(row_ref[...], (width, width))
    vbc_ref[...] = across + across.T
    out_ref[...] = jnp.zeros_like(out_ref)
    rows = lax.broadcasted_iota(jnp.int32, out_ref.shape, 0)
    lanes = lax.broadcasted_iota(jnp.int32, out_ref.shape, 1)
    contract = (((1,), (1,)), ((), ()))

    def step(at, carry):
        place, i, j, k = decode(at)
        other, slot = lax.div(place, slots), lax.rem(place, slots)
        occ_sum = occ[i] + occ[j] + occ[k]

        jk = lax.div(j * occupied + k, teams)
        kj = lax.div(k * occupied + j, teams)
        d_jk = dp_ref[jk]
        d_kj = dp_ref[kj]

        def one(a, total):
            block = integrals_ref[i, a]
            left = jnp.concatenate([block, d_jk], axis=1)
            right = jnp.concatenate([d_kj, block], axis=1)
            connected = lax.dot_general(left, right, contract, preferred_element_type=jnp.float32)
            full = connected + singles[i, a] * cp_ref[jk].astype(jnp.float32)
            denominator = (occ_sum - vir[q * blocks + a]) - vbc_ref[...]
            value = full * full / denominator
            return total + jnp.sum(value.reshape(width // 8, 8, width), axis=0)

        total = lax.fori_loop(0, blocks, one, jnp.zeros((8, width), jnp.float32), unroll=unroll)
        here = jnp.logical_and(rows == other, lanes == slot)
        out_ref[...] += jnp.where(here, jnp.sum(total, axis=(0, 1), keepdims=True), 0.0)
        return carry

    lax.fori_loop(0, count, step, 0)


def reduce_kernel(n, groups, slots, part_ref, trip_ref, mean_ref, blk_buf, grp_buf, send_sem, recv_sem, gsend_sem, grecv_sem,
                  stage_ref):
    g = lax.axis_index("grp")
    q = lax.axis_index("blk")
    barrier = pltpu.get_barrier_semaphore()
    for dg in range(1, groups):
        pl.semaphore_signal(barrier, inc=1, device_id={"grp": (g + dg) % groups}, device_id_type=MESH)
    for dq in range(1, n):
        pl.semaphore_signal(barrier, inc=1, device_id={"blk": (q + dq) % n}, device_id_type=MESH)
    pl.semaphore_wait(barrier, groups - 1 + n - 1)
    copies = []
    for dq in range(1, n):
        copy = pltpu.make_async_remote_copy(
            src_ref=part_ref, dst_ref=blk_buf.at[q], send_sem=send_sem.at[dq - 1], recv_sem=recv_sem.at[dq - 1],
            device_id={"blk": (q + dq) % n}, device_id_type=MESH)
        copy.start()
        copies.append(copy)
    blk_buf[q] = part_ref[...]
    for copy in copies:
        copy.wait()
    stage = jnp.sum(blk_buf[...], axis=0)
    stage_ref[...] = stage
    grp_buf[g] = stage
    copies = []
    for dg in range(1, groups):
        copy = pltpu.make_async_remote_copy(
            src_ref=stage_ref, dst_ref=grp_buf.at[g], send_sem=gsend_sem.at[dg - 1], recv_sem=grecv_sem.at[dg - 1],
            device_id={"grp": (g + dg) % groups}, device_id_type=MESH)
        copy.start()
        copies.append(copy)
    for copy in copies:
        copy.wait()
    table = jnp.sum(grp_buf[...], axis=0)
    rows = lax.broadcasted_iota(jnp.int32, table.shape, 0)
    trip_ref[...] = jnp.sum(jnp.where(rows == g, table, 0.0), axis=0, keepdims=True)
    mean_ref[...] = jnp.sum(table, keepdims=True) / (groups * slots)


def body(n, groups, integrals, doubles, coulomb, singles, occ_energy, vir_energy, triplets, tile_count):
    occupied, _, width, _ = integrals.shape
    rows = doubles.shape[0]
    slots = triplets.shape[1]
    teams = team_count(occupied, rows, groups)
    runs = rows // teams
    pairs = n * runs
    f32, i32 = jnp.float32, jnp.int32
    vmem = pl.BlockSpec(memory_space=pltpu.VMEM)
    smem = pl.BlockSpec(memory_space=pltpu.SMEM)
    hbm = pl.BlockSpec(memory_space=pltpu.HBM)
    dma = pltpu.SemaphoreType.DMA

    row_bytes = pairs * width * width * doubles.dtype.itemsize
    spare = 1 << 20
    keep = integrals.size * integrals.dtype.itemsize + 2 * row_bytes + 2 * spare
    lanes = -(-slots // 128) * 128
    length = -(-groups * slots // 128) * 128

    packed = jax.ShapeDtypeStruct((pairs, width, width), doubles.dtype)
    dp, cp, held, listed, counts = pl.pallas_call(
        functools.partial(gather_kernel, n, groups, teams, occupied, slots),
        out_shape=(packed, packed, jax.ShapeDtypeStruct(integrals.shape, integrals.dtype), jax.ShapeDtypeStruct((1, length), i32), jax.ShapeDtypeStruct((1, 128), i32)),
        in_specs=[hbm, hbm, hbm, hbm, smem],
        out_specs=(vmem, vmem, vmem, vmem, vmem),
        scratch_shapes=[
            pltpu.VMEM((groups, 1, lanes), i32), pltpu.VMEM((3, 1, slots), i32), dma, dma, dma((runs, 2)), dma((runs, 2, n - 1)), dma((runs, 2, n - 1)), dma((runs, 2, n - 1)), dma((runs, 2, n - 1)),
            dma((groups - 1,)), dma((groups - 1,)),
        ],
        compiler_params=pltpu.CompilerParams(collective_id=0, has_side_effects=True, vmem_limit_bytes=keep),
        name="gather",
    )(*(pltpu.with_memory_space_constraint(x, pltpu.HBM)
        for x in (doubles, coulomb, integrals, jnp.transpose(triplets, (2, 0, 1)))), tile_count)

    blocks = integrals.shape[1]
    part = pl.pallas_call(
        functools.partial(compute_kernel, groups, slots, teams, occupied, blocks),
        out_shape=jax.ShapeDtypeStruct((groups, slots), f32),
        in_specs=[smem, smem, smem, smem, smem, vmem, vmem, vmem, vmem],
        out_specs=vmem,
        scratch_shapes=[pltpu.VMEM((width, width), f32)],
        compiler_params=pltpu.CompilerParams(vmem_limit_bytes=keep),
        name="energy",
    )(listed, counts, singles, occ_energy, vir_energy, held, dp, cp, vir_energy.reshape(1, width))

    trip, mean = pl.pallas_call(
        functools.partial(reduce_kernel, n, groups, slots),
        out_shape=(jax.ShapeDtypeStruct((1, slots), f32), jax.ShapeDtypeStruct((1, 1), f32)),
        in_specs=[vmem],
        out_specs=(vmem, vmem),
        scratch_shapes=[
            pltpu.VMEM((n, groups, slots), f32), pltpu.VMEM((groups, groups, slots), f32),
            dma((n - 1,)), dma((n - 1,)), dma((groups - 1,)), dma((groups - 1,)), pltpu.VMEM((groups, slots), f32),
        ],
        compiler_params=pltpu.CompilerParams(collective_id=1, has_side_effects=True, vmem_limit_bytes=4 * spare),
        name="join",
    )(part)
    return trip, mean.reshape(())


def solution(mesh):
    in_specs = (
        P(None, "blk", None, None),
        P("blk", None, None),
        P("blk", None, None),
        P(None, "blk"),
        P(),
        P(),
        P("grp", None, None),
        P("grp"),
    )
    out_specs = (P("grp", None), P())
    step = functools.partial(body, mesh.shape["blk"], mesh.shape["grp"])
    return jax.shard_map(step, mesh=mesh, in_specs=in_specs, out_specs=out_specs, check_vma=False)
```
